32 devices in a mesh: seq: 2 (over x), expert: 16 (over z, y, core).
Axes of the slice: x: 2, y: 2, z: 4, core: 2. Of those that a mesh axis runs over, the one named last changes fastest.
Arguments:
- tokens: bfloat16 [768, 7168], P('expert', 'seq'), may hold values from -6 to 6
- expert_ids: int32 [768, 8], P('expert'), may hold values from 0 to 15, all different within a row
- route_weights: float32 [768, 8], P('expert'), may hold values from 0.05 to 1
- capacity: int32 [16], replicated, may hold values from 6 to 12
- expert_gate_up: bfloat16 [16, 2, 1024, 7168], P('expert', None, 'seq'), may hold values from -0.0625 to 0.0625
- expert_down: bfloat16 [16, 1024, 7168], P('expert', None, 'seq'), may hold values from -0.1875 to 0.1875
Outputs:
- mixed: bfloat16 [768, 7168], P('expert', 'seq')
The draws below stay inside these ranges and needn't reach their ends.
Inputs may be any that keep to these rules, and one draw needn't show every extreme that they name: `expert_ids`: each row names 8 different experts.
All inputs are finite; a program needn't handle non-finite values.
Results may differ from the reference program's by a relative error of at most 0.02.
Values may be sent and summed in bfloat16 or wider, within the bound.
No kernel may reach another device: no remote copies, remote signals or barrier semaphores. Data moves between devices by JAX's collectives and lax.ppermute only.
A program may use at most 128 MiB of HBM per device.

```python
import math
import jax
import jax.numpy as jnp
from jax import lax

D = 7168
TOP = 8
FF = 1024
TG = 48
CAP = 12
EXPERTS = 16
TOKENS = 768
N_SEQ = 2


def place_ends(result, rng, least, largest):
    extent = result.shape
    index_at = [jax.random.randint(jax.random.fold_in(rng, axis), (), 0, extent[axis]) for axis in range(len(extent))]
    result = result.at[tuple(index_at)].set(least)
    longest = extent.index(max(extent))
    index_at[longest] = (index_at[longest] + 1) % extent[longest]
    return result.at[tuple(index_at)].set(largest)


def shard_levels(stream_key, dims, shards, smallest, largest):
    loudness, own = 1.0, jax.random.fold_in(stream_key, 6)
    for dim, shards_of in shards:
        draws = jnp.exp(jax.random.uniform(jax.random.fold_in(own, dim), (shards_of,), jnp.float32, smallest / len(shards), largest / len(shards)))
        loudness = loudness * jnp.repeat(draws, dims[dim] // shards_of).reshape([-1 if axis == dim else 1 for axis in range(len(dims))])
    return loudness


def choose_distinct(own_key, rows, count, top, lift):
    ranking = jax.random.permutation(jax.random.fold_in(own_key, 1), count)
    boost = ranking
    for power in range(3):
        boost = boost * boost // count
    boost = boost * lift // count
    lots = jax.random.randint(jax.random.fold_in(own_key, 2), (rows, count), 0, 4096) + boost
    sure = jax.random.permutation(jax.random.fold_in(own_key, 3), rows)[jnp.arange(count) % rows]
    lots = jnp.where(jnp.arange(rows)[:, None] == sure[None, :], 1 << 14, lots)
    score = lots * count + jnp.arange(count)
    return lax.top_k(score.astype(jnp.int32), top)[1].astype(jnp.int32)


def gaussian(own_key, shape, scale, bound, shards=(), kind=jnp.bfloat16):
    gain = shard_levels(own_key, shape, shards, -0.22, 0.18) if shards else 1.0
    array = jax.random.normal(own_key, shape, jnp.float32) * scale * gain
    return jnp.minimum(jnp.maximum(array, -bound), bound).astype(kind)


def setup_inputs(seed: int = 0) -> dict:
    seeds = jax.random.split(jax.random.key(seed), 7)
    tokens = gaussian(seeds[0], (TOKENS, D), 1.0, 6.0, ((0, 16), (1, 2)))
    expert_ids = choose_distinct(seeds[1], TOKENS, EXPERTS, TOP, 8192)
    route_weights = jnp.clip(jnp.exp(math.log(1.0) - 2.9957323 * jax.random.uniform(seeds[2], (TOKENS, TOP), jnp.float32) ** shard_levels(seeds[2], (TOKENS, TOP), ((0, 16),), -0.2, 0.2)), 0.05, 1.0)
    capacity = place_ends(jax.random.randint(seeds[3], (EXPERTS,), max(1, CAP // 2), CAP + 1), jax.random.fold_in(seeds[3], 1), max(1, CAP // 2), CAP).astype(jnp.int32)
    expert_gate_up = gaussian(seeds[4], (EXPERTS, 2, FF, D), D ** -0.5, 0.0625, ((0, 16), (2, 2)))
    expert_down = gaussian(seeds[5], (EXPERTS, FF, D), FF ** -0.5, 0.1875, ((0, 16), (2, 2)))
    return {"tokens": tokens, "expert_ids": expert_ids, "route_weights": route_weights, "capacity": capacity, "expert_gate_up": expert_gate_up, "expert_down": expert_down}


def reference(tokens, expert_ids, route_weights, capacity, expert_gate_up, expert_down):
    token_count = tokens.shape[0]
    width = tokens.shape[1]
    top_count = expert_ids.shape[1]
    expert_count = capacity.shape[0]
    group_count = token_count // TG
    assign = TG * top_count
    block_width = width // N_SEQ
    flat_ids = expert_ids.reshape(group_count, assign)
    one_hot = (flat_ids[:, :, None] == jnp.arange(expert_count, dtype=jnp.int32)[None, None, :]).astype(jnp.int32)
    within = jnp.sum((jnp.cumsum(one_hot, axis=1) - one_hot) * one_hot, axis=2).astype(jnp.int32)
    retained = within < capacity[flat_ids]
    token_index = (jnp.arange(group_count, dtype=jnp.int32)[:, None] * TG
                   + jnp.arange(assign, dtype=jnp.int32)[None, :] // top_count).astype(jnp.int32)
    group_index = jnp.broadcast_to(jnp.arange(group_count, dtype=jnp.int32)[:, None], (group_count, assign))
    target = jnp.where(retained, flat_ids, expert_count).astype(jnp.int32)
    place = jnp.minimum(within, CAP - 1).astype(jnp.int32)
    table = jnp.full((expert_count, group_count, CAP), token_count, jnp.int32)
    table = table.at[target, group_index, place].set(token_index, mode="drop")
    padded = jnp.concatenate([tokens, jnp.zeros((1, width), jnp.bfloat16)], axis=0)
    weight_flat = jnp.where(retained, route_weights.reshape(group_count, assign), 0.0).astype(jnp.float32)
    column = (group_index * CAP + within).astype(jnp.int32)
    column = jnp.where(retained, column, group_count * CAP).astype(jnp.int32)

    def project(rows, weight):
        blocks = rows.reshape(rows.shape[0], N_SEQ, block_width)
        wblocks = weight.astype(jnp.float32).reshape(weight.shape[0], N_SEQ, block_width)
        partial_value = jnp.einsum("nsd,fsd->snf", blocks, wblocks)
        rounded = lax.optimization_barrier(partial_value.astype(jnp.bfloat16))
        return jnp.sum(rounded.astype(jnp.float32), axis=0)

    def one_expert(total, expert):
        rows = padded[table[expert].reshape(-1)].astype(jnp.float32)
        gate = project(rows, expert_gate_up[expert, 0])
        up = project(rows, expert_gate_up[expert, 1])
        hidden = (jax.nn.silu(gate) * up).astype(jnp.bfloat16)
        output = jnp.dot(hidden.astype(jnp.float32), expert_down[expert].astype(jnp.float32),
                         preferred_element_type=jnp.float32).astype(jnp.bfloat16)
        select = jnp.where(flat_ids == expert, weight_flat, 0.0).astype(jnp.float32)
        mixing = jnp.zeros((token_count, group_count * CAP), jnp.float32)
        mixing = mixing.at[token_index.reshape(-1), column.reshape(-1)].add(select.reshape(-1), mode="drop")
        total = total + jnp.dot(mixing, output.astype(jnp.float32), precision=lax.Precision.HIGHEST)
        return total, None

    total, _ = lax.scan(one_expert, jnp.zeros((token_count, width), jnp.float32),
                        jnp.arange(expert_count, dtype=jnp.int32))
    return total.astype(jnp.bfloat16)
```

```python
import functools

import jax
import jax.numpy as jnp
from jax import lax
from jax.experimental import pallas as pl
from jax.experimental.pallas import tpu as pltpu
from jax.sharding import PartitionSpec as P

CAP = 12
VMEM = pl.BlockSpec(memory_space=pltpu.VMEM)
SMEM = pl.BlockSpec(memory_space=pltpu.SMEM)


def shifts(count):
    if count & (count - 1) == 0:
        return list(range(count - 1, -1, -1)), lambda unit, d: unit ^ d
    return list(range(count - 1, -1, -1)), lambda unit, d: (unit + d) % count


def place_kernel(pair, units, xor, where_ref, capacity_ref, meta_a, meta_b, tok_a, tok_b, *outs):
    mix_ref, blocks = outs[0], outs[1:]
    unit, member = where_ref[0], where_ref[1]
    top = meta_a.shape[1] // 2
    rows = tok_a.shape[0]
    total = rows * pair
    metas = [meta_a[...], meta_b[...]][:pair]
    meta = jnp.concatenate(metas, axis=0).T
    ids, weights = meta[:top], meta[top:]
    offset = lax.broadcasted_iota(jnp.int32, (units, 1), 0)
    if xor:
        target = unit ^ offset
    else:
        target = lax.rem(unit + offset, units)
    expert = target * pair + member
    expert_f = expert.astype(jnp.float32)
    chosen = jnp.zeros((units, total), jnp.float32)
    weight = jnp.zeros((units, total), jnp.float32)
    for k in range(top):
        hit = ids[k : k + 1] == expert_f
        chosen = jnp.where(hit, 1.0, chosen)
        weight = jnp.where(hit, weights[k : k + 1], weight)
    before = lax.broadcasted_iota(jnp.int32, (total, total), 0)
    after = lax.broadcasted_iota(jnp.int32, (total, total), 1)
    order = jnp.logical_and(before < after, (before >= rows) == (after >= rows))
    rank = jnp.dot(
        chosen.astype(jnp.bfloat16), order.astype(jnp.bfloat16), preferred_element_type=jnp.float32
    )
    experts = capacity_ref.shape[1]
    lane = lax.broadcasted_iota(jnp.int32, (units, experts), 1)
    limit = jnp.sum(
        jnp.where(lane == expert, capacity_ref[...], 0).astype(jnp.float32), axis=1, keepdims=True
    )
    column = lax.broadcasted_iota(jnp.int32, (units, total), 1)
    base = jnp.where(column >= rows, float(CAP), 0.0)
    kept = jnp.logical_and(chosen > 0.0, rank < limit)
    key = jnp.where(kept, rank + base, -1.0)
    height = CAP * pair
    slot = lax.broadcasted_iota(jnp.int32, (units, height, total), 1).astype(jnp.float32)
    match = key[:, None, :] == slot
    mix_ref[...] = jnp.where(match, weight[:, None, :], 0.0).reshape(units * height, total)
    placing = jnp.where(match, 1.0, 0.0).reshape(units * height, total).astype(jnp.bfloat16)
    toks = [tok_a[...], tok_b[...]][:pair]
    token = jnp.concatenate(toks, axis=0)
    out = jnp.dot(placing, token, preferred_element_type=jnp.float32).astype(jnp.bfloat16)
    for d in range(units):
        blocks[d][...] = out[d * height : (d + 1) * height]


def mix_kernel(own_rows, mix_ref, *refs):
    own_ref, other_ref = refs[-2], refs[-1]
    back = jnp.concatenate([r[...] for r in refs[:-2]], axis=0)
    mix = mix_ref[...]
    total = None
    for _ in range(3):
        part = mix.astype(jnp.bfloat16)
        mix = mix - part.astype(jnp.float32)
        term = lax.dot_general(
            part, back, (((0,), (0,)), ((), ())), preferred_element_type=jnp.float32
        )
        total = term if total is None else total + term
    own_ref[...] = total[:own_rows]
    other_ref[...] = total[own_rows:].astype(jnp.bfloat16)


def gate_up_kernel(first, last, *refs):
    refs = list(refs)
    refs.pop(0)
    rows_scratch = refs.pop()
    out_ref = refs.pop()
    acc_ref = None if first else refs.pop()
    weight = refs.pop()
    step = pl.program_id(0)

    @pl.when(step == 0)
    def _():
        at = 0
        for r in refs:
            rows_scratch[at : at + r.shape[0], :] = r[...]
            at += r.shape[0]

    dims = (((1,), (1,)), ((), ()))
    gate = lax.dot_general(
        rows_scratch[...], weight[0], dims, preferred_element_type=jnp.float32
    )
    up = lax.dot_general(rows_scratch[...], weight[1], dims, preferred_element_type=jnp.float32)
    if not first:
        gate = gate + acc_ref[0]
        up = up + acc_ref[1]
    if last:
        out_ref[...] = (gate / (1.0 + jnp.exp(-gate)) * up).astype(jnp.bfloat16)
    else:
        out_ref[0] = gate
        out_ref[1] = up


def gate_up(blocks, weights, acc, index, last):
    hidden_share = weights.shape[1]
    share = blocks[0].shape[1]
    count = sum(b.shape[0] for b in blocks)
    tile = 128 if hidden_share % 128 == 0 else hidden_share
    whole = [pl.BlockSpec(b.shape, lambda i, s: (0, 0)) for b in blocks]
    acc_spec = pl.BlockSpec((2, count, tile), lambda i, s: (0, 0, i))
    if last:
        out_shape = jax.ShapeDtypeStruct((count, hidden_share), jnp.bfloat16)
        out_spec = pl.BlockSpec((count, tile), lambda i, s: (0, i))
    else:
        out_shape = jax.ShapeDtypeStruct((2, count, hidden_share), jnp.float32)
        out_spec = acc_spec
    return pl.pallas_call(
        functools.partial(gate_up_kernel, acc is None, last),
        out_shape=out_shape,
        grid_spec=pltpu.PrefetchScalarGridSpec(
            num_scalar_prefetch=1,
            grid=(hidden_share // tile,),
            in_specs=whole
            + [pl.BlockSpec((2, tile, share), lambda i, s: (0, i, s[0]))]
            + ([] if acc is None else [acc_spec]),
            out_specs=out_spec,
            scratch_shapes=[pltpu.VMEM((count, share), jnp.bfloat16)],
        ),
        cost_estimate=pl.CostEstimate(
            flops=4 * count * share * hidden_share,
            bytes_accessed=4 * share * hidden_share,
            transcendentals=0,
        ),
        name="gate_up_last" if last else "gate_up",
    )(index, *blocks, weights, *([] if acc is None else [acc]))


def down_kernel(height, index_ref, *refs):
    refs = list(refs)
    outs = []
    n_hidden = index_ref.shape[0]
    hidden = refs[:n_hidden]
    weight = refs[n_hidden]
    outs = refs[n_hidden + 1 :]
    total = None
    for m in range(n_hidden):
        size = hidden[m].shape[1]
        start = pl.multiple_of(index_ref[m] * size, size)
        term = jnp.dot(
            hidden[m][...], weight[pl.ds(start, size), :], preferred_element_type=jnp.float32
        )
        total = term if total is None else total + term
    total = total.astype(jnp.bfloat16)
    for d, out in enumerate(outs):
        out[...] = total[d * height : (d + 1) * height]


def down_project(hidden, weights, index, units):
    count = hidden[0].shape[0]
    width = weights.shape[1]
    tile = 512 if width % 512 == 0 else width
    height = count // units
    return pl.pallas_call(
        functools.partial(down_kernel, height),
        out_shape=[jax.ShapeDtypeStruct((height, width), jnp.bfloat16)] * units,
        grid_spec=pltpu.PrefetchScalarGridSpec(
            num_scalar_prefetch=1,
            grid=(width // tile,),
            in_specs=[pl.BlockSpec(h.shape, lambda i, s: (0, 0)) for h in hidden]
            + [pl.BlockSpec((weights.shape[0], tile), lambda i, s: (0, i))],
            out_specs=[pl.BlockSpec((height, tile), lambda i, s: (0, i))] * units,
        ),
        cost_estimate=pl.CostEstimate(
            flops=2 * count * weights.shape[0] * width,
            bytes_accessed=2 * weights.shape[0] * width,
            transcendentals=0,
        ),
        name="down",
    )(index, *hidden, weights)


def body(sizes, tokens, expert_ids, route_weights, capacity, expert_gate_up, expert_down):
    n_seq, n_expert = sizes
    pair = 2 if n_expert % 2 == 0 else 1
    units = n_expert // pair
    far_first, move = shifts(units)
    xor = units & (units - 1) == 0
    rows, share = tokens.shape
    experts = capacity.shape[0]
    e_index = lax.axis_index("expert")
    s_index = lax.axis_index("seq")
    where = jnp.stack([e_index // pair, e_index % pair]).astype(jnp.int32)
    swap = [(e, e ^ 1) for e in range(n_expert)]

    meta = jnp.concatenate([expert_ids.astype(jnp.float32), route_weights], axis=1)
    if pair == 2:
        meta_other = lax.ppermute(meta, "expert", swap)
        tokens_other = lax.ppermute(tokens, "expert", swap)
    else:
        meta_other, tokens_other = meta, tokens
    height = CAP * pair
    mix, *blocks = pl.pallas_call(
        functools.partial(place_kernel, pair, units, xor),
        out_shape=[jax.ShapeDtypeStruct((units * height, rows * pair), jnp.float32)]
        + [jax.ShapeDtypeStruct((height, share), jnp.bfloat16)] * units,
        in_specs=[SMEM, VMEM, VMEM, VMEM, VMEM, VMEM],
        out_specs=[VMEM] * (units + 1),
        name="place",
    )(where, capacity.reshape(1, experts), meta, meta_other, tokens, tokens_other)

    def send(block, d):
        return lax.ppermute(
            block,
            "expert",
            [(e, move(e // pair, d) * pair + e % pair) for e in range(n_expert)],
        )

    def send_back(block, d):
        return lax.ppermute(
            block,
            "expert",
            [(move(e // pair, d) * pair + e % pair, e) for e in range(n_expert)],
        )

    received = {0: blocks[0]}
    for d in far_first:
        if d:
            received[d] = send(blocks[d], d)
    near_first = far_first[::-1]
    own = [received[d] for d in range(units)]
    weights = expert_gate_up[0]
    if share % 128 == 0 and n_seq == 2:
        across = [(0, 1), (1, 0)]
        crossed = {d: lax.ppermute(received[d], "seq", across) for d in near_first}
        other = [crossed[d] for d in range(units)]
        mine = s_index.astype(jnp.int32).reshape(1)
        acc = gate_up(own, weights, None, mine, False)
        hidden = gate_up(other, weights, acc, 1 - mine, True)
        hidden_other = lax.ppermute(hidden, "seq", across)
        both = jnp.concatenate([mine, 1 - mine])
        outputs = down_project([hidden, hidden_other], expert_down[0], both, units)
    else:
        piece = lax.all_gather(jnp.concatenate(own, axis=0), "seq", axis=1, tiled=True)
        gate_up_value = jnp.einsum(
            "rs,gfs->grf", piece, weights, preferred_element_type=jnp.float32
        )
        hidden = (jax.nn.silu(gate_up_value[0]) * gate_up_value[1]).astype(jnp.bfloat16)
        hidden = lax.all_gather(hidden, "seq", axis=1, tiled=True)
        result = jnp.dot(hidden, expert_down[0], preferred_element_type=jnp.float32)
        result = result.astype(jnp.bfloat16)
        outputs = [result[d * height : (d + 1) * height] for d in range(units)]

    back = {0: outputs[0]}
    for d in far_first:
        if d:
            back[d] = send_back(outputs[d], d)
    own_part, other_part = pl.pallas_call(
        functools.partial(mix_kernel, rows),
        out_shape=[
            jax.ShapeDtypeStruct((rows, share), jnp.float32),
            jax.ShapeDtypeStruct((rows * (pair - 1) or 8, share), jnp.bfloat16),
        ],
        in_specs=[VMEM] * (units + 1),
        out_specs=[VMEM] * 2,
        name="mix",
    )(mix, *[back[d] for d in range(units)])
    if pair == 2:
        arrived = lax.ppermute(other_part, "expert", swap)
        own_part = own_part + arrived.astype(jnp.float32)
    return own_part.astype(jnp.bfloat16)


def solution(mesh):
    sizes = (mesh.shape["seq"], mesh.shape["expert"])
    in_specs = (
        P("expert", "seq"),
        P("expert", None),
        P("expert", None),
        P(),
        P("expert", None, "seq", None),
        P("expert", None, "seq"),
    )
    out_specs = P("expert", "seq")
    return jax.shard_map(
        functools.partial(body, sizes),
        mesh=mesh,
        in_specs=in_specs,
        out_specs=out_specs,
        check_vma=False,
    )
```
